32 devices in a mesh: dp: 2 (over x), expert: 16 (over z, y, core).
Axes of the slice: x: 2, y: 2, z: 4, core: 2. Of those that a mesh axis runs over, the one named last changes fastest.
Arguments:
- queries: bfloat16 [1024, 4, 3072], P('expert', 'dp'), may hold values from -256 to 256
- key_nope: bfloat16 [1024, 4, 2048], P('expert', 'dp'), may hold values from -4 to 4
- key_rope: bfloat16 [1024, 4, 64], P('expert', 'dp'), may hold values from -4 to 4
- values: bfloat16 [1024, 4, 2048], P('expert', 'dp'), may hold values from -6 to 6
- residual: bfloat16 [1024, 4, 2048], P('expert', 'dp'), may hold values from -6 to 6
- segments: int32 [4, 1024], P('dp'), may hold values from 0 to 1, never falling along the last dimension, each value on 1 to 768 neighbouring positions
- out_proj: bfloat16 [2048, 2048], P(('dp', 'expert')), may hold values from -0.125 to 0.125
- norm_gain: bfloat16 [2048], replicated, may hold values from 0.5 to 1.5
- expert_gate: bfloat16 [16, 2048, 704], P('expert'), may hold values from -0.125 to 0.125
- expert_up: bfloat16 [16, 2048, 704], P('expert'), may hold values from -0.125 to 0.125
- expert_down: bfloat16 [16, 704, 2048], P('expert'), may hold values from -0.21875 to 0.21875
- routes: int32 [2, 16, 128, 6], P('dp', 'expert'), may hold values from 0 to 15, all different within a row; in each aligned block of 128 rows (0 to 127, 128 to 255, ..., all dimensions but the last counted through in order) at most 72 rows name the same one
- route_weights: float32 [2, 16, 128, 6], P('dp', 'expert'), may hold values from 0.1 to 0.6
Outputs:
- layer_out: bfloat16 [1024, 4, 2048], P('expert', 'dp')
The draws below stay inside these ranges and needn't reach their ends.
Inputs may be any that keep to these rules, and one draw needn't show every extreme that they name: `routes`: each row names 6 different experts; within the rows of one device no expert is named more than 72 times.
All inputs are finite; a program needn't handle non-finite values.
Results may differ from the reference program's by a relative error of at most 0.0049.
Values may be sent and summed in bfloat16 or wider, within the bound.
A program may use at most 128 MiB of HBM per device.

```python
import math
import jax
import jax.numpy as jnp
import numpy as np
from jax import lax

D = 2048
HEADS = 16
NOPE = 128
ROPE = 64
V_DIM = 128
FF_E = 704
TOP = 6
STREAMS = 2
DOCS = 2
TOK_HALF = 64
QK_DIM = 192
EXPERTS = 16
LENGTH = 1024
S_ALL = 4
TOK_DEV = 128
MOST = 72
DOC_MOST = 768
N_DP = 2
N_EXPERT = 16


def key_parts(key):
    nope_part = jnp.clip(jax.random.normal(jax.random.fold_in(key, 11), (LENGTH, S_ALL, HEADS * NOPE), jnp.float32), -4.0, 4.0)
    rope_part = jnp.clip(jax.random.normal(jax.random.fold_in(key, 12), (LENGTH, S_ALL, ROPE), jnp.float32), -4.0, 4.0)
    return (nope_part, rope_part)


def draw_key_nope(key, part):
    return key_parts(key)[0].astype(jnp.bfloat16)


def draw_key_rope(key, part):
    return key_parts(key)[1].astype(jnp.bfloat16)


def draw_queries(key, part):
    drawn = jnp.clip(jax.random.normal(jax.random.fold_in(key, 15), (LENGTH, S_ALL, HEADS * QK_DIM), jnp.float32), -6.0, 6.0)
    return drawn.astype(jnp.bfloat16)


def steps_of(key, dims, shards, smallest, largest):
    def one(axis_at, shards_of):
        heights = jax.random.uniform(jax.random.fold_in(jax.random.fold_in(key, 6), axis_at), (shards_of,), jnp.float32, smallest / len(shards), largest / len(shards))
        return jnp.repeat(jnp.exp(heights), dims[axis_at] // shards_of).reshape((-1,) + (1,) * (len(dims) - axis_at - 1))

    loudness = one(*shards[0])
    for cut in shards[1:]:
        loudness = loudness * one(*cut)
    return loudness


def profile(amount, total, bound, skew):
    portions = [(1 << 20) // math.isqrt(rank ** skew) + 1 for rank in range(2, amount + 1)]
    surplus, given = total - bound - (amount - 1), [1] * (amount - 1)
    while surplus > 0:
        movable = [i for i in range(amount - 1) if given[i] < bound]
        mass, budget = sum([portions[i] for i in movable]), surplus
        for i in movable:
            more = min(bound - given[i], max(1, budget * portions[i] // mass), surplus)
            given[i] = given[i] + more
            surplus = surplus - more
    return np.array([bound] + given)


def uneven(own_key, count, total, most, lean):
    if count == 2:
        one = jax.random.randint(own_key, (), max(1, total - most), min(most, total - 1) + 1)
        return jnp.stack([one, total - one])
    sizes = jnp.asarray(profile(count, total, most, lean), jnp.int32)
    twos = (count - 1) // 2
    giver, receiver = sizes[1:1 + 2 * twos:2], sizes[2:2 + 2 * twos:2]
    slack = jnp.minimum(giver - 1, most - receiver)
    passed = jax.random.randint(jax.random.fold_in(own_key, 1), (twos,), 0, 1 << 20) % (slack + 1)
    sizes = sizes.at[1:1 + 2 * twos:2].set(giver - passed).at[2:2 + 2 * twos:2].set(receiver + passed)
    return sizes[jax.random.permutation(jax.random.fold_in(own_key, 2), count)]


def routed_block(key, own, number, rows, count, top, most, slope):
    ranking = jax.random.permutation(key, count)
    heavy_load, usual = portions_of(count, rows * top, most, slope, True), portions_of(count, rows * top, most, slope, False)
    places = jnp.arange(count)

    def named(lengths, rotation):
        used = int((lengths > 0).sum())
        fixed = max(1, used // 4)
        passed = fixed + (places - fixed + rotation * (used - fixed)) % max(1, count - fixed)
        return jnp.zeros((count,), jnp.int32).at[ranking[jnp.where(places < fixed, places, passed)]].set(jnp.asarray(lengths, jnp.int32))

    lengths = jnp.where(number % 4 == 0, named(heavy_load, number // 4), named(usual, number - number // 4 - 1))
    mixed = jax.random.permutation(jax.random.fold_in(own, 3), count)
    source_of, receiver = mixed[0:count // 2 * 2:2], mixed[1:count // 2 * 2:2]
    margin = jnp.minimum(lengths[source_of] - 1, most - lengths[receiver]) // 2
    margin = jnp.where((source_of == ranking[0]) | (receiver == ranking[0]) | (lengths[receiver] == 0), 0, jnp.maximum(margin, 0))
    passed = jax.random.randint(jax.random.fold_in(own, 4), (count // 2,), 0, 1 << 20) % (margin + 1)
    lengths = lengths.at[source_of].add(-passed).at[receiver].add(passed)
    labels = jnp.searchsorted(jnp.cumsum(lengths), jnp.arange(rows * top), side="right").astype(jnp.int32)
    grid = labels.reshape(top, rows).T
    grid = grid[jax.random.permutation(jax.random.fold_in(own, 1), rows)]
    rotation = jax.random.randint(jax.random.fold_in(own, 2), (rows, 1), 0, top)
    return jnp.take_along_axis(grid, (jnp.arange(top)[None, :] + rotation) % top, axis=1)


def portions_of(number_of, total, most, lean, full):
    loads = [(1 << 20) // math.isqrt(standing ** lean) + 1 for standing in range(1, number_of + 1)]
    largest = most if full else min(most, max(-(-total // number_of), total * loads[0] // sum(loads)))
    least = 1 if total - largest >= number_of - 1 else 0
    counts, surplus = [largest] + [least] * (number_of - 1), total - largest - least * (number_of - 1)
    while surplus > 0:
        free = [i for i in range(1, number_of) if counts[i] < largest] or [i for i in range(1, number_of) if counts[i] < most]
        pool, left = sum([loads[i] for i in free]), surplus
        for i in free:
            extra = min(most - counts[i], max(1, left * loads[i] // pool), surplus)
            counts[i] = counts[i] + extra
            surplus = surplus - extra
    return np.array(counts)


def normal_values(own_key, extent, scale, most, shards=(), held_as=jnp.bfloat16):
    values = scale * jax.random.normal(own_key, extent, jnp.float32)
    if shards:
        values = values * steps_of(own_key, extent, shards, -0.22, 0.18)
    return jnp.clip(values, -most, most).astype(held_as)


def setup_inputs(seed: int = 0) -> dict:
    streams_of = jax.random.split(jax.random.key(seed), 14)
    queries = draw_queries(jax.random.fold_in(streams_of[13], 71), 0)
    key_nope = draw_key_nope(jax.random.fold_in(streams_of[13], 71), 0)
    key_rope = draw_key_rope(jax.random.fold_in(streams_of[13], 71), 0)
    values = normal_values(streams_of[3], (LENGTH, S_ALL, HEADS * V_DIM), 1.0, 6.0, ((0, 16), (1, 2)))
    residual = normal_values(streams_of[4], (LENGTH, S_ALL, D), 1.0, 6.0, ((0, 16), (1, 2)))
    segments = jax.vmap(lambda own: jnp.searchsorted(jnp.cumsum(uneven(own, DOCS, LENGTH, DOC_MOST, 1)), jnp.arange(LENGTH), side="right"))(jax.random.split(streams_of[5], S_ALL)).reshape((S_ALL, LENGTH)).astype(jnp.int32)
    out_proj = normal_values(streams_of[6], (HEADS * V_DIM, D), (HEADS * V_DIM) ** -0.5, 0.125, ((0, 32),))
    norm_gain = jnp.clip(1.0 + 0.1 * jax.random.normal(streams_of[7], (D,), jnp.float32), 0.5, 1.5).astype(jnp.bfloat16)
    expert_gate = normal_values(streams_of[8], (EXPERTS, D, FF_E), D ** -0.5, 0.125, ((0, 16),))
    expert_up = normal_values(streams_of[9], (EXPERTS, D, FF_E), D ** -0.5, 0.125, ((0, 16),))
    expert_down = normal_values(streams_of[10], (EXPERTS, FF_E, D), FF_E ** -0.5, 0.21875, ((0, 16),))
    routes_keys = jax.random.split(jax.random.fold_in(streams_of[11], 1), N_DP * N_EXPERT * TOK_DEV // TOK_DEV)
    routes_turns = jax.random.permutation(jax.random.fold_in(streams_of[11], 3), N_DP * N_EXPERT * TOK_DEV // TOK_DEV)
    routes = jax.vmap(lambda own, number: routed_block(jax.random.fold_in(streams_of[11], 2), own, number, TOK_DEV, EXPERTS, TOP, MOST, 1))(routes_keys, routes_turns).reshape((N_DP, N_EXPERT, TOK_DEV, TOP))
    route_weights = jnp.clip(0.1 + 0.5 * jax.random.uniform(streams_of[12], (N_DP, N_EXPERT, TOK_DEV, TOP), jnp.float32) ** steps_of(streams_of[12], (N_DP, N_EXPERT, TOK_DEV, TOP), ((0, 2), (1, 16)), -0.2, 0.2), 0.1, 0.6)
    return dict(queries=queries, key_nope=key_nope, key_rope=key_rope, values=values, residual=residual, segments=segments, out_proj=out_proj, norm_gain=norm_gain, expert_gate=expert_gate, expert_up=expert_up, expert_down=expert_down, routes=routes, route_weights=route_weights)


EPSILON = 1e-06

def to_streams(block_array):
    width = block_array.shape[-1]
    shaped = block_array.reshape(N_DP, N_EXPERT, TOK_HALF, STREAMS, width)
    shaped = jnp.transpose(shaped, (1, 2, 0, 3, 4))
    return shaped.reshape(LENGTH, S_ALL, width)

def feed_forward(rows, gate_matrix, up_matrix, down_matrix):
    gate_part = jnp.dot(rows, gate_matrix, preferred_element_type=jnp.float32)
    up_part = jnp.dot(rows, up_matrix, preferred_element_type=jnp.float32)
    activated = (jax.nn.silu(gate_part) * up_part).astype(jnp.bfloat16)
    return jnp.dot(activated, down_matrix, preferred_element_type=jnp.float32).astype(jnp.bfloat16)

def attend_stream(inputs):
    query_rows, nope_rows, rope_rows, value_rows, segment_row = inputs
    query_heads = query_rows.reshape(LENGTH, HEADS, QK_DIM).astype(jnp.float32)
    key_heads = jnp.concatenate([nope_rows.reshape(LENGTH, HEADS, NOPE), jnp.broadcast_to(rope_rows[:, None, :], (LENGTH, HEADS, ROPE))], axis=2).astype(jnp.float32)
    value_heads = value_rows.reshape(LENGTH, HEADS, V_DIM).astype(jnp.float32)
    scores = jnp.einsum('qhd,khd->hqk', query_heads, key_heads) * QK_DIM ** (-0.5)
    positions = jnp.arange(LENGTH, dtype=jnp.int32)
    allowed = (positions[:, None] >= positions[None, :]) & (segment_row[:, None] == segment_row[None, :])
    scores = jnp.where(allowed[None], scores, -jnp.inf)
    row_peak = lax.optimization_barrier(jnp.max(scores, axis=2, keepdims=True))
    raised = jnp.exp(scores - row_peak)
    probs = (raised / lax.optimization_barrier(jnp.sum(raised, axis=2, keepdims=True))).astype(jnp.bfloat16)
    mixed = jnp.einsum('hqk,khd->qhd', probs.astype(jnp.float32), value_heads)
    return mixed.reshape(LENGTH, HEADS * V_DIM).astype(jnp.bfloat16)

def reference(queries, key_nope, key_rope, values, residual, segments, out_proj, norm_gain, expert_gate, expert_up, expert_down, routes, route_weights):
    inputs = (jnp.swapaxes(queries, 0, 1), jnp.swapaxes(key_nope, 0, 1), jnp.swapaxes(key_rope, 0, 1), jnp.swapaxes(values, 0, 1), segments)
    attended = lax.map(attend_stream, inputs)
    token_count = LENGTH * S_ALL
    attn_rows = jnp.swapaxes(attended, 0, 1).reshape(token_count, HEADS * V_DIM)
    projected = jnp.dot(attn_rows, out_proj, preferred_element_type=jnp.float32)
    hidden = residual.reshape(token_count, D).astype(jnp.float32) + projected
    mean_square = lax.optimization_barrier(jnp.mean(hidden * hidden, axis=1, keepdims=True))
    normed = (hidden * lax.rsqrt(mean_square + EPSILON) * norm_gain.astype(jnp.float32)).astype(jnp.bfloat16)
    chosen = to_streams(routes).reshape(token_count, TOP)
    scales = to_streams(route_weights).reshape(token_count, TOP)
    capacity = min(N_DP * N_EXPERT * MOST, token_count)
    row_ids = jnp.arange(token_count, dtype=jnp.int32)

    def one_expert(routed_total, expert_inputs):
        gate_matrix, up_matrix, down_matrix, expert_id = expert_inputs
        matches = chosen == expert_id
        picked = jnp.any(matches, axis=1)
        weight_row = lax.optimization_barrier(jnp.sum(jnp.where(matches, scales, jnp.zeros_like(scales)), axis=1))
        live_order = (jnp.cumsum(picked.astype(jnp.int32)) - 1).astype(jnp.int32)
        live_place = jnp.where(picked, live_order, capacity).astype(jnp.int32)
        source_rows = jnp.zeros((capacity,), jnp.int32).at[live_place].set(row_ids, mode='drop')
        filled = jnp.zeros((capacity,), jnp.int32).at[live_place].set(1, mode='drop')
        outputs = feed_forward(normed[source_rows], gate_matrix, up_matrix, down_matrix)
        contribution = (filled > 0)[:, None] * weight_row[source_rows][:, None] * outputs.astype(jnp.float32)
        return (routed_total.at[source_rows].add(contribution), expert_id)
    expert_ids = jnp.arange(EXPERTS, dtype=jnp.int32)
    routed_total = lax.scan(one_expert, jnp.zeros((token_count, D), jnp.float32), (expert_gate, expert_up, expert_down, expert_ids))[0]
    layer_out = (hidden + routed_total).astype(jnp.bfloat16)
    return layer_out.reshape(LENGTH, S_ALL, D)
```

```python
import jax
import jax.numpy as jnp
from jax import lax
from jax.sharding import PartitionSpec as P

HEADS = 16
NOPE = 128
ROPE = 64
V_DIM = 128
TOP = 6


EPSILON = 1e-06
QUERY_BLOCK = 512


def feed_forward(rows, gate_matrix, up_matrix, down_matrix):
    gate_part = jnp.dot(rows, gate_matrix, preferred_element_type=jnp.float32)
    up_part = jnp.dot(rows, up_matrix, preferred_element_type=jnp.float32)
    activated = (jax.nn.silu(gate_part) * up_part).astype(jnp.bfloat16)
    return jnp.dot(activated, down_matrix, preferred_element_type=jnp.float32).astype(jnp.bfloat16)


def attend_items(query_items, key_items, value_items, segment_items):
    length, count_items, qk_width = query_items.shape
    block_rows = QUERY_BLOCK
    score_scale = qk_width ** (-0.5)
    key_positions = jnp.arange(length, dtype=jnp.int32)

    def one_block(block_index):
        first_row = block_index * block_rows
        query_block = lax.dynamic_slice_in_dim(query_items, first_row, block_rows, 0)
        scores = (
            jnp.einsum("qid,kid->iqk", query_block, key_items, preferred_element_type=jnp.float32)
            * score_scale
        )
        row_positions = first_row + jnp.arange(block_rows, dtype=jnp.int32)
        row_segments = lax.dynamic_slice_in_dim(segment_items, first_row, block_rows, 1)
        allowed = (row_positions[None, :, None] >= key_positions[None, None, :]) & (
            row_segments[:, :, None] == segment_items[:, None, :]
        )
        scores = jnp.where(allowed, scores, -jnp.inf)
        row_peak = jnp.max(scores, axis=2, keepdims=True)
        raised = jnp.exp(scores - row_peak)
        weights = (raised / jnp.sum(raised, axis=2, keepdims=True)).astype(jnp.bfloat16)
        return jnp.einsum(
            "iqk,kid->qid", weights, value_items, preferred_element_type=jnp.float32
        ).astype(jnp.bfloat16)

    blocks = lax.map(one_block, jnp.arange(length // block_rows, dtype=jnp.int32))
    return blocks.reshape(length, count_items, value_items.shape[2])


def body(
    queries,
    key_nope,
    key_rope,
    values,
    residual,
    segments,
    out_proj,
    norm_gain,
    expert_gate,
    expert_up,
    expert_down,
    routes,
    route_weights,
):
    half_rows, stream_count, query_width = queries.shape
    model_width = residual.shape[2]
    token_rows = half_rows * stream_count
    expert_count = lax.axis_size("expert")
    item_count = stream_count * HEADS // expert_count
    key_heads = jnp.concatenate(
        [
            key_nope.reshape(half_rows, stream_count, HEADS, NOPE),
            jnp.broadcast_to(key_rope[:, :, None, :], (half_rows, stream_count, HEADS, ROPE)),
        ],
        axis=3,
    )
    query_items = queries.reshape(half_rows, stream_count * HEADS, NOPE + ROPE)
    key_items = key_heads.reshape(half_rows, stream_count * HEADS, NOPE + ROPE)
    value_items = values.reshape(half_rows, stream_count * HEADS, V_DIM)
    packed = jnp.concatenate([query_items, key_items, value_items], axis=2)
    packed_all = lax.all_to_all(packed, "expert", split_axis=1, concat_axis=0, tiled=True)
    qk_width = NOPE + ROPE
    query_all = packed_all[:, :, :qk_width]
    key_all = packed_all[:, :, qk_width : 2 * qk_width]
    value_all = packed_all[:, :, 2 * qk_width :]
    item_ids = lax.axis_index("expert") * item_count + jnp.arange(item_count, dtype=jnp.int32)
    stream_ids = item_ids // HEADS
    selector = (stream_ids[:, None] == jnp.arange(stream_count, dtype=jnp.int32)[None, :]).astype(
        jnp.int32
    )
    segment_items = jnp.sum(selector[:, :, None] * segments[None, :, :], axis=1)
    attended_items = attend_items(query_all, key_all, value_all, segment_items)
    attended_back = lax.all_to_all(
        attended_items, "expert", split_axis=0, concat_axis=1, tiled=True
    )
    attn_rows = attended_back.reshape(token_rows, HEADS * V_DIM)
    projected = jnp.dot(
        attn_rows,
        lax.all_gather(out_proj, ("dp", "expert"), axis=0, tiled=True),
        preferred_element_type=jnp.float32,
    )
    hidden = residual.reshape(token_rows, model_width).astype(jnp.float32) + projected
    mean_square = jnp.mean(hidden * hidden, axis=1, keepdims=True)
    normed = (hidden * lax.rsqrt(mean_square + EPSILON) * norm_gain.astype(jnp.float32)).astype(
        jnp.bfloat16
    )
    token_routes = routes.reshape(token_rows, TOP)
    token_weights = route_weights.reshape(token_rows, TOP)
    expert_ids = jnp.arange(expert_count, dtype=jnp.int32)
    weight_table = jnp.sum(
        jnp.where(
            token_routes[:, :, None] == expert_ids[None, None, :], token_weights[:, :, None], 0.0
        ),
        axis=1,
    )
    own_weights = lax.all_to_all(
        weight_table.T, "expert", split_axis=0, concat_axis=0, tiled=True
    ).reshape(expert_count * token_rows, 1)
    all_rows = lax.all_gather(normed, "expert", axis=0, tiled=True)
    results = feed_forward(all_rows, expert_gate[0], expert_up[0], expert_down[0])
    partial = (own_weights * results.astype(jnp.float32)).astype(jnp.bfloat16)
    routed_sum = lax.psum_scatter(partial, "expert", scatter_dimension=0, tiled=True).astype(
        jnp.float32
    )
    layer_out = (hidden + routed_sum).astype(jnp.bfloat16)
    return layer_out.reshape(half_rows, stream_count, model_width)


def solution(mesh):
    return jax.shard_map(
        body,
        mesh=mesh,
        in_specs=(
            P("expert", "dp", None),
            P("expert", "dp", None),
            P("expert", "dp", None),
            P("expert", "dp", None),
            P("expert", "dp", None),
            P("dp", None),
            P(("dp", "expert"), None),
            P(),
            P("expert", None, None),
            P("expert", None, None),
            P("expert", None, None),
            P("dp", "expert", None, None),
            P("dp", "expert", None, None),
        ),
        out_specs=P("expert", "dp", None),
        check_vma=False,
    )
```

```python
import jax
import jax.numpy as jnp
from jax import lax
from jax.experimental import pallas as pl
from jax.experimental.pallas import tpu as pltpu
from jax.sharding import PartitionSpec as P

HEADS = 16
NOPE = 128
ROPE = 64
V_DIM = 128
TOP = 6


EPSILON = 1e-06
QUERY_BLOCK = 256
CHUNKS = 2
ITEM_WIDTH = 2 * (NOPE + ROPE) + V_DIM


def feed_forward(rows, gate_matrix, up_matrix, down_matrix):
    gate_part = jnp.dot(rows, gate_matrix, preferred_element_type=jnp.float32)
    up_part = jnp.dot(rows, up_matrix, preferred_element_type=jnp.float32)
    activated = (jax.nn.silu(gate_part) * up_part).astype(jnp.bfloat16)
    return jnp.dot(activated, down_matrix, preferred_element_type=jnp.float32).astype(jnp.bfloat16)


def attend_kernel(packed_ref, segment_row_ref, segment_column_ref, attended_ref):
    length, packed_width = packed_ref.shape
    block_rows = min(QUERY_BLOCK, length)
    score_scale = (NOPE + ROPE) ** (-0.5)
    contract_last = (((1,), (1,)), ((), ()))
    for item in range(packed_width // ITEM_WIDTH):
        base = item * ITEM_WIDTH
        for first_row in range(0, length, block_rows):
            key_count = first_row + block_rows
            rows = pl.ds(first_row, block_rows)
            keys = pl.ds(0, key_count)
            rope_at = base + 2 * NOPE + V_DIM
            query_rope = packed_ref[rows, rope_at : rope_at + 2 * ROPE][:, :ROPE]
            key_rope = packed_ref[keys, rope_at : rope_at + 2 * ROPE][:, ROPE:]
            scores = lax.dot_general(
                packed_ref[rows, base : base + NOPE],
                packed_ref[keys, base + NOPE : base + 2 * NOPE],
                contract_last,
                preferred_element_type=jnp.float32,
            ) + lax.dot_general(
                query_rope, key_rope, contract_last, preferred_element_type=jnp.float32
            )
            scores = scores * score_scale
            row_positions = first_row + lax.broadcasted_iota(jnp.int32, scores.shape, 0)
            key_positions = lax.broadcasted_iota(jnp.int32, scores.shape, 1)
            allowed = (row_positions >= key_positions) & (
                segment_column_ref[rows, :] == segment_row_ref[:, keys]
            )
            scores = jnp.where(allowed, scores, -jnp.inf)
            row_peak = jnp.max(scores, axis=1, keepdims=True)
            raised = jnp.exp(scores - row_peak)
            weights = (raised / jnp.sum(raised, axis=1, keepdims=True)).astype(jnp.bfloat16)
            attended_ref[rows, item * V_DIM : (item + 1) * V_DIM] = jnp.dot(
                weights,
                packed_ref[keys, base + 2 * NOPE : base + 2 * NOPE + V_DIM],
                preferred_element_type=jnp.float32,
            ).astype(jnp.bfloat16)


def attend_items(packed_rows, segment_row):
    length, packed_width = packed_rows.shape
    item_count = packed_width // ITEM_WIDTH
    vmem = pl.BlockSpec(memory_space=pltpu.VMEM)
    return pl.pallas_call(
        attend_kernel,
        out_shape=jax.ShapeDtypeStruct((length, item_count * V_DIM), jnp.bfloat16),
        in_specs=[vmem] * 3,
        out_specs=vmem,
        cost_estimate=pl.CostEstimate(
            flops=item_count * length * length * (NOPE + ROPE + V_DIM),
            bytes_accessed=2 * length * packed_width,
            transcendentals=item_count * length * length // 2,
        ),
    )(packed_rows, segment_row.reshape(1, length), segment_row.reshape(length, 1))


def body(
    queries,
    key_nope,
    key_rope,
    values,
    residual,
    segments,
    out_proj,
    norm_gain,
    expert_gate,
    expert_up,
    expert_down,
    routes,
    route_weights,
):
    half_rows, stream_count, query_width = queries.shape
    model_width = residual.shape[2]
    token_rows = half_rows * stream_count
    expert_count = lax.axis_size("expert")
    item_count = stream_count * HEADS // expert_count
    query_heads = queries.reshape(half_rows, stream_count, HEADS, NOPE + ROPE)
    head_shape = (half_rows, stream_count, HEADS, ROPE)
    packed = jnp.concatenate(
        [
            query_heads[..., :NOPE],
            key_nope.reshape(half_rows, stream_count, HEADS, NOPE),
            values.reshape(half_rows, stream_count, HEADS, V_DIM),
            query_heads[..., NOPE:],
            jnp.broadcast_to(key_rope[:, :, None, :], head_shape),
        ],
        axis=3,
    ).reshape(half_rows, expert_count, item_count * ITEM_WIDTH)
    packed_all = lax.all_to_all(
        packed.transpose(1, 0, 2), "expert", split_axis=0, concat_axis=0, tiled=True
    )
    length = expert_count * half_rows
    own_stream = lax.axis_index("expert") * item_count // HEADS
    selector = (jnp.arange(stream_count, dtype=jnp.int32) == own_stream).astype(jnp.int32)
    segment_row = jnp.sum(selector[:, None] * segments, axis=0)
    attended_items = attend_items(
        packed_all.reshape(length, item_count * ITEM_WIDTH), segment_row
    )
    attended_back = lax.all_to_all(
        attended_items.reshape(expert_count, half_rows, item_count * V_DIM),
        "expert",
        split_axis=0,
        concat_axis=0,
        tiled=True,
    )
    attn_rows = (
        attended_back.reshape(
            stream_count, expert_count // stream_count, half_rows, item_count * V_DIM
        )
        .transpose(2, 0, 1, 3)
        .reshape(token_rows, HEADS * V_DIM)
    )
    projected = jnp.dot(
        attn_rows,
        lax.all_gather(out_proj, ("dp", "expert"), axis=0, tiled=True),
        preferred_element_type=jnp.float32,
    )
    hidden = residual.reshape(token_rows, model_width).astype(jnp.float32) + projected
    mean_square = jnp.mean(hidden * hidden, axis=1, keepdims=True)
    normed = (hidden * lax.rsqrt(mean_square + EPSILON) * norm_gain.astype(jnp.float32)).astype(
        jnp.bfloat16
    )
    token_routes = routes.reshape(token_rows, TOP)
    token_weights = route_weights.reshape(token_rows, TOP)
    expert_ids = jnp.arange(expert_count, dtype=jnp.int32)
    weight_table = jnp.sum(
        jnp.where(
            token_routes[:, :, None] == expert_ids[None, None, :], token_weights[:, :, None], 0.0
        ),
        axis=1,
    )
    own_weights = lax.all_to_all(
        weight_table.T, "expert", split_axis=0, concat_axis=0, tiled=True
    ).reshape(expert_count, token_rows)
    chunk_rows = token_rows // CHUNKS
    routed_chunks = []
    for chunk in range(CHUNKS):
        part = slice(chunk * chunk_rows, (chunk + 1) * chunk_rows)
        all_rows = lax.all_gather(normed[part], "expert", axis=0, tiled=True)
        results = feed_forward(all_rows, expert_gate[0], expert_up[0], expert_down[0])
        scale = own_weights[:, part].reshape(expert_count * chunk_rows, 1)
        partial = (scale * results.astype(jnp.float32)).astype(jnp.bfloat16)
        routed_chunks.append(
            lax.psum_scatter(partial, "expert", scatter_dimension=0, tiled=True)
        )
    routed_sum = jnp.concatenate(routed_chunks, axis=0).astype(jnp.float32)
    layer_out = (hidden + routed_sum).astype(jnp.bfloat16)
    return layer_out.reshape(half_rows, stream_count, model_width)


def solution(mesh):
    return jax.shard_map(
        body,
        mesh=mesh,
        in_specs=(
            P("expert", "dp", None),
            P("expert", "dp", None),
            P("expert", "dp", None),
            P("expert", "dp", None),
            P("expert", "dp", None),
            P("dp", None),
            P(("dp", "expert"), None),
            P(),
            P("expert", None, None),
            P("expert", None, None),
            P("expert", None, None),
            P("dp", "expert", None, None),
            P("dp", "expert", None, None),
        ),
        out_specs=P("expert", "dp", None),
        check_vma=False,
    )
```
